8 devices in a mesh: data: 2 (over z, y), expert: 4 (over x, core).
Axes of the slice: x: 2, y: 2, z: 1, core: 2. Of those that a mesh axis runs over, the one named last changes fastest.
Arguments:
- x: bfloat16 [16384, 4096], P(('data', 'expert')), parts along dimension 0
- idx: int32 [16384, 2], P(('data', 'expert')), parts along dimension 0
- wr: bfloat16 [4096, 8], replicated
- w1: bfloat16 [8, 4096, 6400], P('expert')
- w3: bfloat16 [8, 4096, 6400], P('expert')
- w2: bfloat16 [8, 6400, 4096], P('expert')
Outputs:
- output: bfloat16 [16384, 4096], P(('data', 'expert')), parts along dimension 0
There are 2 independent parts. The reference program is written for one: setup_inputs(seed, part) draws one part's arguments, and reference() takes and returns one part's arrays. A program takes and returns all parts, laid end to end along the dimension named above; an argument that names none is the same for every part.
All inputs are finite; a program needn't handle non-finite values.
Results may differ from the reference program's by a relative error of at most 0.001.
Values are sent between devices in bfloat16 or wider.
A program may use at most 1.5 GiB of HBM per device.

```python
import jax
import jax.numpy as jnp
from jax import lax

N = 4
T = 2048
D = 4096
FF = 6400
TOP = 2
E = 8
CS = 1024


def _routing(key):
    h = E // 2

    def one(k):
        kh, kp, ks = jax.random.split(k, 3)
        hot = jax.random.permutation(kh, E)[:h]
        p = jax.random.permutation(kp, T)
        e0 = hot[p % h]
        e1 = (e0 + 1 + (p // h) % (E - 1)) % E
        pair = jnp.stack([e0, e1], axis=1)
        swap = jax.random.bernoulli(ks, 0.5, (T, 1))
        return jnp.where(swap, pair[:, ::-1], pair)
    return jax.vmap(one)(jax.random.split(key, N)).reshape(N * T, TOP).astype(jnp.int32)


def setup_inputs(seed: int = 0, part: int = 0) -> dict:
    key = jax.random.key(seed)
    kshared, kpart = jax.random.split(key)
    kx, ki = jax.random.split(jax.random.fold_in(kpart, part))
    kr, k1, k3, k2 = jax.random.split(kshared, 4)
    x = jax.random.normal(kx, (N * T, D), jnp.float32).astype(jnp.bfloat16)
    wr = (jax.random.normal(kr, (D, E), jnp.float32) * (1.5 * D ** -0.5)).astype(jnp.bfloat16)
    w1 = (jax.random.normal(k1, (E, D, FF), jnp.float32) * D ** -0.5).astype(jnp.bfloat16)
    w3 = (jax.random.normal(k3, (E, D, FF), jnp.float32) * D ** -0.5).astype(jnp.bfloat16)
    w2 = (jax.random.normal(k2, (E, FF, D), jnp.float32) * FF ** -0.5).astype(jnp.bfloat16)
    return {'x': x, 'idx': _routing(jax.random.fold_in(ki, 7)), 'wr': wr, 'w1': w1, 'w3': w3, 'w2': w2}


def reference(x, idx, wr, w1, w3, w2):
    logits = jnp.dot(x, wr, preferred_element_type=jnp.float32)
    g = jax.nn.softmax(jnp.take_along_axis(logits, idx, axis=1), axis=-1)
    e = idx.reshape(N, T * TOP)
    oh = (e[:, :, None] == jnp.arange(E, dtype=jnp.int32)[None, None, :]).astype(jnp.int32)
    pos = jnp.take_along_axis(jnp.cumsum(oh, axis=1), e[:, :, None], axis=2)[:, :, 0] - 1
    src = jnp.arange(N, dtype=jnp.int32)[:, None]
    valid = (pos < CS).reshape(-1)
    dest = jnp.where(valid, ((e * N + src) * CS + pos).reshape(-1), E * N * CS)
    rows = jnp.repeat(x, TOP, axis=0)
    buf = jnp.zeros((E * N * CS, D), jnp.bfloat16).at[dest].set(rows, mode='drop').reshape(E, N * CS, D)

    def expert(args):
        xb, a1, a3, a2 = args
        h1 = jnp.dot(xb, a1, preferred_element_type=jnp.float32)
        h3 = jnp.dot(xb, a3, preferred_element_type=jnp.float32)
        h = (jax.nn.silu(h1) * h3).astype(jnp.bfloat16)
        return jnp.dot(h, a2, preferred_element_type=jnp.float32).astype(jnp.bfloat16)

    o = lax.map(expert, (buf, w1, w3, w2)).reshape(E * N * CS, D)
    op = jnp.where(valid[:, None], o[jnp.where(valid, dest, 0)], 0)
    y = jnp.sum(g[:, :, None] * op.reshape(N * T, TOP, D).astype(jnp.float32), axis=1)
    return y.astype(jnp.bfloat16)
```

```python
import functools

import jax
import jax.numpy as jnp
from jax import lax
from jax.experimental import pallas as pl
from jax.experimental.pallas import tpu as pltpu
from jax.sharding import PartitionSpec as P

VMEM_BYTES = 67043328
LANES = 128
SB = 1024
GRAN = 128
UNIT = 512
TAILS = (128, 256, 384)
CHUNK = 256
CAP = 416
MORE = 152
BN1 = 256
BN2 = 256


def _for_rows(count, fn):
    unit = UNIT // GRAN
    whole = lax.div(count, unit)

    def body(i, c):
        fn(pl.multiple_of(i * UNIT, UNIT), UNIT)
        return c

    lax.fori_loop(0, whole, body, 0)
    rest = count - whole * unit
    for tail in TAILS:
        @pl.when(rest == tail // GRAN)
        def _():
            fn(pl.multiple_of(whole * UNIT, UNIT), tail)


def _ffn_kernel(n1, blk, sub, ex, x_ref, w1_ref, w3_ref, w2_ref, o_ref, h_ref):
    s, j = pl.program_id(0), pl.program_id(1)
    count = sub[s]

    @pl.when(j < n1)
    def _():
        col = pl.multiple_of(j * BN1, BN1)

        def up(r, m):
            x = x_ref[pl.ds(r, m), :]
            a = jnp.dot(x, w1_ref[0], preferred_element_type=jnp.float32)
            b = jnp.dot(x, w3_ref[0], preferred_element_type=jnp.float32)
            h_ref[pl.ds(r, m), pl.ds(col, BN1)] = (a * jax.nn.sigmoid(a) * b).astype(h_ref.dtype)
        _for_rows(count, up)

    @pl.when(j >= n1)
    def _():
        def down(r, m):
            o = jnp.dot(h_ref[pl.ds(r, m), :], w2_ref[0], preferred_element_type=jnp.float32)
            o_ref[pl.ds(r, m), :] = o.astype(o_ref.dtype)
        _for_rows(count, down)


def _ffn(xs, w1, w3, w2, meta, rows_out, rows_hint):
    blk, sub, ex = meta
    d, f = w1.shape[1], w1.shape[2]
    n1, n2 = f // BN1, d // BN2
    at = lambda s, j, sub: jnp.where(sub[s] > 0, j, n1 + n2 - 1)
    up = lambda s, j, sub: jnp.minimum(at(s, j, sub), n1 - 1)
    down = lambda s, j, sub: jnp.maximum(at(s, j, sub) - n1, 0)
    return pl.pallas_call(
        functools.partial(_ffn_kernel, n1),
        out_shape=jax.ShapeDtypeStruct((rows_out, d), xs.dtype),
        grid_spec=pltpu.PrefetchScalarGridSpec(
            num_scalar_prefetch=3,
            grid=(blk.shape[0], n1 + n2),
            in_specs=[
                pl.BlockSpec((SB, d), lambda s, j, blk, sub, ex: (blk[s], 0)),
                pl.BlockSpec((1, d, BN1), lambda s, j, blk, sub, ex: (ex[s], 0, up(s, j, sub))),
                pl.BlockSpec((1, d, BN1), lambda s, j, blk, sub, ex: (ex[s], 0, up(s, j, sub))),
                pl.BlockSpec((1, f, BN2), lambda s, j, blk, sub, ex: (ex[s], 0, down(s, j, sub))),
            ],
            out_specs=pl.BlockSpec((SB, BN2), lambda s, j, blk, sub, ex: (blk[s], down(s, j, sub))),
            scratch_shapes=[pltpu.VMEM((SB, f), xs.dtype)],
        ),
        compiler_params=pltpu.CompilerParams(
            vmem_limit_bytes=VMEM_BYTES, dimension_semantics=("arbitrary", "arbitrary")),
        cost_estimate=pl.CostEstimate(
            flops=6 * rows_hint * d * f, bytes_accessed=12 * d * f, transcendentals=rows_hint * f),
        name="ffn",
    )(blk, sub, ex, xs, w1, w3, w2)


def _unwritten(shape, dtype):
    return pl.pallas_call(
        lambda o: None, out_shape=jax.ShapeDtypeStruct(shape, dtype),
        out_specs=pl.BlockSpec(memory_space=pl.ANY), name="unwritten")()


def _pad8(n):
    return (n + 7) & ~7


def _row_list(incl, off, end, rows):
    c = incl.shape[0]
    r = jnp.arange(rows, dtype=jnp.int32)
    chunk = jnp.sum((end[None, :] <= r[:, None]).astype(jnp.int32), axis=1)
    hot = chunk[:, None] == jnp.arange(c, dtype=jnp.int32)[None, :]
    start = jnp.sum(jnp.where(hot, off[None, :], 0), axis=1)
    cum = jnp.dot(hot.astype(jnp.bfloat16), incl.astype(jnp.bfloat16), preferred_element_type=jnp.float32)
    lane = jnp.sum((cum <= (r - start).astype(jnp.float32)[:, None]).astype(jnp.int32), axis=1)
    return jnp.minimum(chunk * LANES + lane, c * LANES - 1)


def _meta(counts, per):
    epd = counts.shape[0]
    i = jnp.arange(epd * per, dtype=jnp.int32)
    n = jnp.broadcast_to(counts[:, None], (epd, per)).reshape(-1)
    sub = jnp.clip(lax.div(n - lax.rem(i, per) * SB + GRAN - 1, GRAN), 0, SB // GRAN)
    live = sub > 0
    slot = jnp.sum((live[None, :] & (i[None, :] < i[:, None])).astype(jnp.int32), axis=1)
    live_n = jnp.sum(live.astype(jnp.int32))
    put = (slot[None, :] == jnp.minimum(i, live_n - 1)[:, None]) & live[None, :]
    pick = lambda v: jnp.sum(jnp.where(put, v[None, :], 0), axis=1).astype(jnp.int32)
    return pick(i), jnp.where(i < live_n, pick(sub), 0), pick(lax.div(i, per))


def _gather(src, lists, counts, buf):
    epd, cap = lists.shape
    flat = lists.reshape(-1)
    nch = lax.div(counts + CHUNK - 1, CHUNK)
    ends = [jnp.sum(nch[:e + 1]) for e in range(epd)]

    def body(i, buf):
        row = i * CHUNK
        for e in range(1, epd):
            row = jnp.where(i >= ends[e - 1], e * cap + (i - ends[e - 1]) * CHUNK, row)
        rows = lax.dynamic_slice(flat, (row,), (CHUNK,))
        part = src.at[rows].get(mode='promise_in_bounds')
        return lax.dynamic_update_slice(buf, part, (row, 0))

    return lax.fori_loop(0, ends[-1], body, buf)


def solution(mesh):
    n = mesh.shape['expert']

    def local(x, idx, wr, w1, w3, w2):
        t, d = x.shape
        k = idx.shape[1]
        e_all = wr.shape[1]
        epd = w1.shape[0]
        cs = 2 * k * t // e_all
        half = t // 2
        nc = t // LANES
        hc = nc // 2
        me = lax.axis_index('expert')
        sib = me ^ 1
        far = (me ^ 2) & ~1
        i32 = jnp.int32

        idx_t = idx.T
        idx_g = lax.all_gather(idx_t, ('data', 'expert'))
        xg, idx_g = lax.optimization_barrier((x, idx_g))
        idx_all = lax.dynamic_slice_in_dim(idx_g, lax.axis_index('data') * n, n, axis=0)
        x_h = [lax.all_gather(xg[h * half:(h + 1) * half], 'expert', tiled=True) for h in range(2)]
        x_sib = lax.ppermute(x, 'expert', [(i, i + 1 - 2 * (i % 2)) for i in range(n)])

        ids = jnp.arange(e_all, dtype=i32)
        hit = jnp.any(idx_all[:, None, :, :] == ids[None, :, None, None], axis=2)
        hit = hit.reshape(n, e_all, nc, LANES)
        lane = jnp.arange(LANES, dtype=i32)
        tri = (lane[:, None] <= lane[None, :]).astype(jnp.bfloat16)
        incl = jnp.dot(hit.astype(jnp.bfloat16), tri, preferred_element_type=jnp.float32).astype(i32)
        tot = incl[..., LANES - 1]
        ch = jnp.arange(nc, dtype=i32)
        off = jnp.sum(jnp.where(ch[None, :] < ch[:, None], tot[:, :, None, :], 0), axis=3)
        n_h = jnp.stack([jnp.sum(tot[..., :hc], axis=-1), jnp.sum(tot[..., hc:], axis=-1)], axis=1)

        dev = jnp.arange(n, dtype=i32)
        e_dev = lax.div(ids, epd)
        own = e_dev == me
        far_e = (e_dev >> 1) != (me >> 1)
        extra = cs - CAP
        far_base = 2 * epd * cs
        over_base = far_base + 2 * 2 * epd * CAP
        buf_rows = -(-(over_base + 2 * 2 * epd * extra) // SB) * SB

        take1 = lambda a, i: lax.dynamic_index_in_dim(a, i, 0, keepdims=False)
        mine = lambda a: lax.dynamic_slice_in_dim(a, me * epd, epd, axis=1)

        my_off, my_incl = take1(off, me), take1(incl, me)
        my_hit = take1(hit, me).astype(i32)
        rank = (my_incl - my_hit + my_off[:, :, None]).reshape(e_all, t)
        my_n0 = take1(n_h, me)[0]
        second = (jnp.arange(t, dtype=i32) >= half)[None, :]
        cross = ((e_dev ^ me) & 1) == 1
        slot = cross.astype(i32) * epd + lax.rem(ids, epd)
        far_rank = rank - jnp.where(second, my_n0[:, None], 0)
        far_slot = second.astype(i32) * 2 * epd + slot[:, None]
        far_place = jnp.where(far_rank < CAP, far_base + far_slot * CAP + far_rank,
                              over_base + far_slot * extra + far_rank - CAP)
        near_place = jnp.where(own, lax.rem(ids, epd), epd + lax.rem(ids, epd))[:, None] * cs + rank
        place = jnp.where(far_e[:, None], far_place, near_place)
        pos = jnp.sum(jnp.where(idx_t[:, None, :] == ids[None, :, None], place[None], 0), axis=1)

        incl_l, off_l, tot_l = mine(incl), mine(off), mine(tot)
        n_hl = lax.dynamic_slice_in_dim(n_h, me * epd, epd, axis=2)

        def one_source(s):
            a, o, tt = take1(incl_l, s), take1(off_l, s), take1(tot_l, s)
            return jnp.stack([_row_list(a[e], o[e], o[e] + tt[e], cs) for e in range(epd)]), take1(n_hl, s).sum(axis=0)

        def far_half(h):
            sl = slice(h * hc, (h + 1) * hc)
            pick = lambda a: jnp.moveaxis(lax.dynamic_slice_in_dim(a, far, 2, axis=0)[:, :, sl], 0, 1)
            a, tt = pick(incl_l), pick(tot_l)
            cnt = lax.dynamic_slice_in_dim(n_hl, far, 2, axis=0)[:, h]
            o = pick(off_l) - (lax.dynamic_slice_in_dim(n_hl, far, 2, axis=0)[:, 0].T[:, :, None] if h else 0)
            p0 = _pad8(cnt[0])
            o = o + jnp.stack([jnp.zeros_like(p0), p0], axis=1)[:, :, None]
            o = o.reshape(epd, nc)
            end = jnp.concatenate([o[:, 1:], (p0 + cnt[1])[:, None]], axis=1)
            a = a.reshape(epd, nc, LANES)
            lst = jnp.stack([_row_list(a[e], o[e], end[e], 2 * cs) for e in range(epd)])
            return lst + far * half, p0 + cnt[1]

        l_own, c_own = one_source(me)
        l_sib, c_sib = one_source(sib)
        l_far, c_far = zip(far_half(0), far_half(1))

        logits = jnp.dot(x, wr, preferred_element_type=jnp.float32)
        g = jax.nn.softmax(jnp.sum(jnp.where(idx[:, :, None] == ids, logits[:, None, :], 0.0), axis=2), axis=-1)

        hint = t * k * n // e_all * epd // 4
        perm = {m: [(i, i ^ m) for i in range(n)] for m in (1, 2, 3)}

        hit_g = jnp.any(idx_g[:, None, :, :] == ids[:, None, None], axis=2)
        most = jnp.max(jnp.sum(hit_g.reshape(-1, 2, half).astype(i32), axis=2))
        steps = jnp.maximum(lax.div(most - CAP + MORE - 1, MORE), 0)

        def start_of(h, home, e):
            first = jnp.where((home & 1) == 1, _pad8(take1(n_hl, home & ~1)[h, e]), 0)
            return pl.multiple_of(e * 2 * cs + first, 8)

        def pack(o, h, m, lo, size):
            home = me ^ m
            return jnp.concatenate([lax.dynamic_slice(o, (start_of(h, home, e) + lo, 0), (size, d)) for e in range(epd)])

        def far_rows(o, h, m, lo, size):
            return lax.ppermute(pack(o, h, m, lo, size), 'expert', perm[m])

        xs = x_sib.at[l_sib.reshape(-1)].get(mode='promise_in_bounds')
        o_sib = _ffn(xs, w1, w3, w2, _meta(c_sib, cs // SB), epd * cs, hint)
        r_sib = lax.ppermute(o_sib, 'expert', perm[1])
        out, o_far, r_far = [o_sib], [], []
        for h in range(2):
            lst, out = lax.optimization_barrier((l_far[h], out))
            xs = _gather(x_h[h], lst, c_far[h], _unwritten((epd * 2 * cs, d), x.dtype))
            last = _ffn(xs, w1, w3, w2, _meta(c_far[h], 2 * cs // SB), epd * 2 * cs + SB, hint)
            o_far.append(last)
            out = [pack(last, h, m, 0, CAP) for m in (2, 3)]
            r_far.append([lax.ppermute(o, 'expert', perm[m]) for o, m in zip(out, (2, 3))])
        lst, out, r_far[0] = lax.optimization_barrier((l_own, out, r_far[0]))
        xs = x.at[lst.reshape(-1)].get(mode='promise_in_bounds')
        buf = _ffn(xs, w1, w3, w2, _meta(c_own, cs // SB), buf_rows, hint)

        buf = lax.dynamic_update_slice(buf, r_sib, (epd * cs, 0))
        for h in range(2):
            for i in range(2):
                buf = lax.dynamic_update_slice(buf, r_far[h][i], (far_base + (2 * h + i) * epd * CAP, 0))

        def more(step, buf):
            for h in range(2):
                for i, m in enumerate((2, 3)):
                    lo = jnp.minimum(CAP + step * MORE, cs - MORE)
                    got = far_rows(o_far[h], h, m, lo, MORE)
                    for e in range(epd):
                        row = over_base + ((2 * h + i) * epd + e) * extra + lo - CAP
                        buf = lax.dynamic_update_slice(buf, got[e * MORE:(e + 1) * MORE], (row, 0))
            return buf

        buf = lax.fori_loop(0, steps, more, buf)

        op = buf.at[pos.reshape(-1)].get(mode='promise_in_bounds').reshape(k, t, d)
        y = jnp.sum(g.T[:, :, None] * op.astype(jnp.float32), axis=0)
        return y.astype(x.dtype)

    tok = P(('data', 'expert'), None)
    wsp = P('expert', None, None)
    return jax.shard_map(local, mesh=mesh, in_specs=(tok, tok, P(), wsp, wsp, wsp), out_specs=tok, check_vma=False)
```

```python
import functools

import jax
import jax.numpy as jnp
from jax import lax
from jax.experimental import pallas as pl
from jax.experimental.pallas import tpu as pltpu
from jax.sharding import PartitionSpec as P

VMEM_BYTES = 67043328
LANES = 128
SB = 1024
GRAN = 128
UNIT = 512
TAILS = (128, 256, 384)
CHUNK = 256
WIN = 512
CWIN = 144
CAP = 416
MORE = 152
BN1 = 256
BN2 = 256


def _for_rows(count, fn):
    unit = UNIT // GRAN
    whole = lax.div(count, unit)

    def body(i, c):
        fn(pl.multiple_of(i * UNIT, UNIT), UNIT)
        return c

    lax.fori_loop(0, whole, body, 0)
    rest = count - whole * unit
    for tail in TAILS:
        @pl.when(rest == tail // GRAN)
        def _():
            fn(pl.multiple_of(whole * UNIT, UNIT), tail)


def _ffn_kernel(blk, sub, ex, live, x_hbm, w1, w3, w2, o_hbm, xb, hb, wu, wd, ob, xsem, s1, s3, sd, so):
    n1, n2 = w1.shape[2] // BN1, w2.shape[2] // BN2
    count_live = live[0]

    def x_copy(s, slot):
        rows = pl.ds(pl.multiple_of(blk[s] * SB, SB), SB)
        return pltpu.make_async_copy(x_hbm.at[rows, :], xb.at[slot], xsem.at[slot])

    def up_copies(s, t, slot):
        cols = pl.ds(pl.multiple_of(t * BN1, BN1), BN1)
        return (pltpu.make_async_copy(w1.at[ex[s], :, cols], wu.at[slot, 0], s1.at[slot]),
                pltpu.make_async_copy(w3.at[ex[s], :, cols], wu.at[slot, 1], s3.at[slot]))

    def down_copy(s, t, slot):
        cols = pl.ds(pl.multiple_of(t * BN2, BN2), BN2)
        return pltpu.make_async_copy(w2.at[ex[s], :, cols], wd.at[slot], sd.at[slot])

    def out_copy(s, t, slot):
        rows = pl.ds(pl.multiple_of(blk[s] * SB, SB), SB)
        cols = pl.ds(pl.multiple_of(t * BN2, BN2), BN2)
        return pltpu.make_async_copy(ob.at[slot], o_hbm.at[rows, cols], so.at[slot])

    @pl.when(count_live > 0)
    def _():
        x_copy(0, 0).start()
        for c in up_copies(0, 0, 0):
            c.start()

    def superblock(s, carry):
        count = sub[s]
        side = s & 1
        down_copy(s, 0, 0).start()

        @pl.when(s + 1 < count_live)
        def _():
            x_copy(s + 1, 1 - side).start()
        x_copy(s, side).wait()

        def up_step(t, carry):
            slot = (s * n1 + t) & 1
            for c in up_copies(s, t, slot):
                c.wait()
            end = t == n1 - 1
            ns, nt = jnp.where(end, s + 1, s), jnp.where(end, 0, t + 1)

            @pl.when(ns < count_live)
            def _():
                for c in up_copies(ns, nt, 1 - slot):
                    c.start()
            col = pl.multiple_of(t * BN1, BN1)

            def up(r, m):
                x = xb[side, pl.ds(r, m), :]
                a = jnp.dot(x, wu[slot, 0], preferred_element_type=jnp.float32)
                b = jnp.dot(x, wu[slot, 1], preferred_element_type=jnp.float32)
                hb[pl.ds(r, m), pl.ds(col, BN1)] = (a * jax.nn.sigmoid(a) * b).astype(hb.dtype)
            _for_rows(count, up)
            return carry

        lax.fori_loop(0, n1, up_step, 0)

        def down_step(t, carry):
            slot = t & 1
            down_copy(s, t, slot).wait()

            @pl.when(t + 1 < n2)
            def _():
                down_copy(s, t + 1, 1 - slot).start()

            @pl.when(t >= 2)
            def _():
                out_copy(s, t - 2, slot).wait()

            def down(r, m):
                o = jnp.dot(hb[pl.ds(r, m), :], wd[slot], preferred_element_type=jnp.float32)
                ob[slot, pl.ds(r, m), :] = o.astype(ob.dtype)
            _for_rows(count, down)
            out_copy(s, t, slot).start()
            return carry

        lax.fori_loop(0, n2, down_step, 0)
        out_copy(s, n2 - 2, 0).wait()
        out_copy(s, n2 - 1, 1).wait()
        return carry

    lax.fori_loop(0, count_live, superblock, 0)


def _ffn(xs, w1, w3, w2, meta, rows_out, rows_hint):
    d, f = w1.shape[1], w1.shape[2]
    smem = pl.BlockSpec(memory_space=pltpu.SMEM)
    hbm = pl.BlockSpec(memory_space=pl.ANY)
    two = pltpu.SemaphoreType.DMA((2,))
    return pl.pallas_call(
        _ffn_kernel,
        out_shape=jax.ShapeDtypeStruct((rows_out, d), xs.dtype),
        in_specs=[smem] * 4 + [hbm] * 4,
        out_specs=hbm,
        scratch_shapes=[
            pltpu.VMEM((2, SB, d), xs.dtype), pltpu.VMEM((SB, f), xs.dtype), pltpu.VMEM((2, 2, d, BN1), xs.dtype),
            pltpu.VMEM((2, f, BN2), xs.dtype), pltpu.VMEM((2, SB, BN2), xs.dtype), two, two, two, two, two],
        compiler_params=pltpu.CompilerParams(vmem_limit_bytes=VMEM_BYTES),
        cost_estimate=pl.CostEstimate(
            flops=6 * rows_hint * d * f, bytes_accessed=12 * d * f, transcendentals=rows_hint * f),
        name="ffn",
    )(*meta, xs, w1, w3, w2)


def _pad8(n):
    return (n + 7) & ~7


def _row_list(incl, off, end, rows):
    c = incl.shape[0]
    r = lax.broadcasted_iota(jnp.int32, (rows, 1), 0)
    chunk = jnp.sum((end[None, :] <= r).astype(jnp.int32), axis=1, keepdims=True)
    hot = chunk == jnp.arange(c, dtype=jnp.int32)[None, :]
    start = jnp.sum(jnp.where(hot, off[None, :], 0), axis=1, keepdims=True)
    cum = jnp.dot(hot.astype(jnp.bfloat16), incl.astype(jnp.bfloat16), preferred_element_type=jnp.float32)
    lane = jnp.sum((cum <= (r - start).astype(jnp.float32)).astype(jnp.int32), axis=1, keepdims=True)
    return jnp.minimum(chunk * LANES + lane, c * LANES - 1)


def _blocks(counts, per, size):
    epd = counts.shape[0]
    i = jnp.arange(epd * per, dtype=jnp.int32)
    n = jnp.broadcast_to(counts[:, None], (epd, per)).reshape(-1)
    rows = jnp.clip(n - lax.rem(i, per) * size, 0, size)
    live = rows > 0
    slot = jnp.sum((live[None, :] & (i[None, :] < i[:, None])).astype(jnp.int32), axis=1)
    live_n = jnp.sum(live.astype(jnp.int32))
    put = (slot[None, :] == jnp.minimum(i, live_n - 1)[:, None]) & live[None, :]
    pick = lambda v: jnp.sum(jnp.where(put, v[None, :], 0), axis=1).astype(jnp.int32)
    return pick(i), pick(rows), pick(lax.div(i, per)), live_n[None]


def _meta(counts, per):
    blk, rows, ex, live = _blocks(counts, per, SB)
    return blk, lax.div(rows + GRAN - 1, GRAN), ex, live


def _gather_kernel(src, blk, first, last, live, list_ref, x_ref, o_ref, acc):
    i = pl.program_id(0)

    @pl.when(i < live[0])
    def _():
        lst = list_ref[...]
        acc[...] = jnp.zeros_like(acc)

        def window(w, c):
            lo = pl.multiple_of(w * WIN, WIN)
            lane = lax.broadcasted_iota(jnp.int32, (CHUNK, WIN), 1) + lo
            hot = jnp.where(lst == lane, 1.0, 0.0).astype(x_ref.dtype)
            acc[...] += jnp.dot(hot, x_ref[pl.ds(lo, WIN), :], preferred_element_type=jnp.float32)
            return c

        lax.fori_loop(lax.div(first[i], WIN), lax.div(last[i], WIN) + 1, window, 0)
        o_ref[...] = acc[...].astype(o_ref.dtype)


def _gather(x, src, tokens, lists, counts):
    rows, d = lists.shape[0], x.shape[1]
    per = rows // CHUNK // counts.shape[0]
    blk, cnt, _, live = _blocks(counts, per, CHUNK)
    table = lists.reshape(rows // CHUNK, CHUNK)
    at = blk[:, None] == jnp.arange(rows // CHUNK, dtype=jnp.int32)[None, :]
    lo = jnp.sum(jnp.where(at, table[:, 0][None, :], 0), axis=1)
    lane = jnp.arange(CHUNK, dtype=jnp.int32)[None, :]
    full = jnp.clip(jnp.broadcast_to(counts[:, None], (counts.shape[0], per)).reshape(-1)
                    - lax.rem(jnp.arange(rows // CHUNK, dtype=jnp.int32), per) * CHUNK, 0, CHUNK)
    top = jnp.max(jnp.where(lane < full[:, None], table, 0), axis=1)
    hi = jnp.sum(jnp.where(at, top[None, :], 0), axis=1)
    return pl.pallas_call(
        _gather_kernel,
        out_shape=jax.ShapeDtypeStruct((rows, d), x.dtype),
        grid_spec=pltpu.PrefetchScalarGridSpec(
            num_scalar_prefetch=5,
            grid=(rows // CHUNK,),
            in_specs=[pl.BlockSpec((CHUNK, 1), lambda i, src, blk, lo, hi, live: (blk[i], 0)),
                      pl.BlockSpec((tokens, d), lambda i, src, blk, lo, hi, live: (src[0], 0))],
            out_specs=pl.BlockSpec((CHUNK, d), lambda i, src, blk, lo, hi, live: (blk[i], 0)),
            scratch_shapes=[pltpu.VMEM((CHUNK, d), jnp.float32)],
        ),
        compiler_params=pltpu.CompilerParams(vmem_limit_bytes=VMEM_BYTES, dimension_semantics=("arbitrary",)),
        cost_estimate=pl.CostEstimate(flops=6 * rows * WIN * d, bytes_accessed=4 * tokens * d, transcendentals=0),
        name="rows",
    )(src, blk, lo, hi, live, lists, x)


def _combine_kernel(lo, cnt, loc_ref, g_ref, own, sib, f00, f01, f10, f11, y_ref, win, sem):
    b, nb = pl.program_id(0), pl.num_programs(0)
    slots = loc_ref.shape[1]
    epd = slots // 4
    d = y_ref.shape[1]

    def copy(ref, stride, b, k, side):
        row = pl.multiple_of((k % epd) * stride + lo[b * slots + k], 16)
        return pltpu.make_async_copy(ref.at[pl.ds(row, CWIN), :], win.at[side, k], sem.at[side, k])

    def start(b, side):
        stride = own.shape[0] // epd
        for k in range(2 * epd):
            copy(own if k < epd else sib, stride, b, k, side).start()
        for h, pair in enumerate(((f00, f01), (f10, f11))):
            @pl.when((b >= nb // 2) == (h == 1))
            def _():
                for k in range(2 * epd, slots):
                    copy(pair[k // epd - 2], CAP, b, k, side).start()

    side = b & 1

    @pl.when(b == 0)
    def _():
        start(0, 0)

    @pl.when(b + 1 < nb)
    def _():
        start(b + 1, 1 - side)

    for k in range(slots):
        copy(own if k < 2 * epd else f00, 0, b, k, side).wait()

    row = lax.broadcasted_iota(jnp.int32, (LANES, CWIN), 1)
    hots = [jnp.where(loc_ref[:, k:k + 1] == row, 1.0, 0.0).astype(y_ref.dtype) for k in range(slots)]
    step = 512

    def columns(c, carry):
        cols = pl.ds(pl.multiple_of(c * step, step), step)
        y = jnp.zeros((LANES, step), jnp.float32)
        r = lax.broadcasted_iota(jnp.int32, (CWIN, step), 0)
        for k in range(slots):
            w = win[side, k, :, cols].astype(jnp.float32)
            w = jnp.where(r < cnt[b * slots + k], w, 0.0).astype(win.dtype)
            y += g_ref[:, k:k + 1] * jnp.dot(hots[k], w, preferred_element_type=jnp.float32)
        y_ref[:, cols] = y.astype(y_ref.dtype)
        return carry

    lax.fori_loop(0, d // step, columns, 0)


def _combine(lo, cnt, loc, gates, arrays, dtype):
    t, slots = loc.shape
    d = arrays[0].shape[1]
    hbm = pl.BlockSpec(memory_space=pl.ANY)
    return pl.pallas_call(
        _combine_kernel,
        out_shape=jax.ShapeDtypeStruct((t, d), dtype),
        grid_spec=pltpu.PrefetchScalarGridSpec(
            num_scalar_prefetch=2,
            grid=(t // LANES,),
            in_specs=[pl.BlockSpec((LANES, slots), lambda b, lo, cnt: (b, 0))] * 2 + [hbm] * 6,
            out_specs=pl.BlockSpec((LANES, d), lambda b, lo, cnt: (b, 0)),
            scratch_shapes=[pltpu.VMEM((2, slots, CWIN, d), dtype), pltpu.SemaphoreType.DMA((2, slots))],
        ),
        compiler_params=pltpu.CompilerParams(vmem_limit_bytes=VMEM_BYTES, dimension_semantics=("arbitrary",)),
        name="combine",
    )(lo, cnt, loc, gates, *arrays)


def solution(mesh):
    n = mesh.shape['expert']

    def local(x, idx, wr, w1, w3, w2):
        t, d = x.shape
        k = idx.shape[1]
        e_all = wr.shape[1]
        epd = w1.shape[0]
        cs = 2 * k * t // e_all
        half = t // 2
        nc = t // LANES
        hc = nc // 2
        me = lax.axis_index('expert')
        sib = me ^ 1
        far = (me ^ 2) & ~1
        i32 = jnp.int32

        idx_t = idx.T
        idx_g = lax.all_gather(idx_t, ('data', 'expert'))
        xg, idx_g = lax.optimization_barrier((x, idx_g))
        idx_all = lax.dynamic_slice_in_dim(idx_g, lax.axis_index('data') * n, n, axis=0)
        x_h = [lax.all_gather(xg[h * half:(h + 1) * half], 'expert', tiled=True) for h in range(2)]
        x_sib = lax.ppermute(x, 'expert', [(i, i + 1 - 2 * (i % 2)) for i in range(n)])

        ids = jnp.arange(e_all, dtype=i32)
        hit = jnp.any(idx_all[:, None, :, :] == ids[None, :, None, None], axis=2)
        hit = hit.reshape(n, e_all, nc, LANES)
        lane = jnp.arange(LANES, dtype=i32)
        tri = (lane[:, None] <= lane[None, :]).astype(jnp.bfloat16)
        incl = jnp.dot(hit.astype(jnp.bfloat16), tri, preferred_element_type=jnp.float32).astype(i32)
        tot = incl[..., LANES - 1]
        ch = jnp.arange(nc, dtype=i32)
        off = jnp.sum(jnp.where(ch[None, :] < ch[:, None], tot[:, :, None, :], 0), axis=3)
        n_h = jnp.stack([jnp.sum(tot[..., :hc], axis=-1), jnp.sum(tot[..., hc:], axis=-1)], axis=1)

        dev = jnp.arange(n, dtype=i32)
        e_dev = lax.div(ids, epd)
        own = e_dev == me
        far_e = (e_dev >> 1) != (me >> 1)
        extra = cs - CAP
        far_base = 2 * epd * cs
        over_base = far_base + 2 * 2 * epd * CAP
        buf_rows = -(-(over_base + 2 * 2 * epd * extra) // SB) * SB

        take1 = lambda a, i: lax.dynamic_index_in_dim(a, i, 0, keepdims=False)
        mine = lambda a: lax.dynamic_slice_in_dim(a, me * epd, epd, axis=1)

        my_off, my_incl = take1(off, me), take1(incl, me)
        my_hit = take1(hit, me).astype(i32)
        rank = (my_incl - my_hit + my_off[:, :, None]).reshape(e_all, t)
        my_n0 = take1(n_h, me)[0]
        second = (jnp.arange(t, dtype=i32) >= half)[None, :]
        cross = ((e_dev ^ me) & 1) == 1
        slot = cross.astype(i32) * epd + lax.rem(ids, epd)
        far_rank = rank - jnp.where(second, my_n0[:, None], 0)
        far_slot = second.astype(i32) * 2 * epd + slot[:, None]
        far_place = jnp.where(far_rank < CAP, far_base + far_slot * CAP + far_rank,
                              over_base + far_slot * extra + far_rank - CAP)
        near_place = jnp.where(own, lax.rem(ids, epd), epd + lax.rem(ids, epd))[:, None] * cs + rank
        place = jnp.where(far_e[:, None], far_place, near_place)
        pos = jnp.sum(jnp.where(idx_t[:, None, :] == ids[None, :, None], place[None], 0), axis=1)

        incl_l, off_l, tot_l = mine(incl), mine(off), mine(tot)
        n_hl = lax.dynamic_slice_in_dim(n_h, me * epd, epd, axis=2)

        def one_source(s):
            a, o, tt = take1(incl_l, s), take1(off_l, s), take1(tot_l, s)
            return jnp.concatenate([_row_list(a[e], o[e], o[e] + tt[e], cs) for e in range(epd)]), take1(n_hl, s).sum(axis=0)

        def far_half(h):
            sl = slice(h * hc, (h + 1) * hc)
            pick = lambda a: jnp.moveaxis(lax.dynamic_slice_in_dim(a, far, 2, axis=0)[:, :, sl], 0, 1)
            a, tt = pick(incl_l), pick(tot_l)
            cnt = lax.dynamic_slice_in_dim(n_hl, far, 2, axis=0)[:, h]
            o = pick(off_l) - (lax.dynamic_slice_in_dim(n_hl, far, 2, axis=0)[:, 0].T[:, :, None] if h else 0)
            p0 = _pad8(cnt[0])
            o = o + jnp.stack([jnp.zeros_like(p0), p0], axis=1)[:, :, None]
            o = o.reshape(epd, nc)
            end = jnp.concatenate([o[:, 1:], (p0 + cnt[1])[:, None]], axis=1)
            a = a.reshape(epd, nc, LANES)
            lst = jnp.concatenate([_row_list(a[e], o[e], end[e], 2 * cs) for e in range(epd)])
            return lst, p0 + cnt[1]

        l_own, c_own = one_source(me)
        l_sib, c_sib = one_source(sib)
        l_far, c_far = zip(far_half(0), far_half(1))

        logits = jnp.dot(x, wr, preferred_element_type=jnp.float32)
        g = jax.nn.softmax(jnp.sum(jnp.where(idx[:, :, None] == ids, logits[:, None, :], 0.0), axis=2), axis=-1)

        hint = t * k * n // e_all * epd // 4
        perm = {m: [(i, i ^ m) for i in range(n)] for m in (1, 2, 3)}

        hit_g = jnp.any(idx_g[:, None, :, :] == ids[:, None, None], axis=2)
        most = jnp.max(jnp.sum(hit_g.reshape(-1, 2, half).astype(i32), axis=2))
        steps = jnp.maximum(lax.div(most - CAP + MORE - 1, MORE), 0)

        def start_of(h, home, e):
            first = jnp.where((home & 1) == 1, _pad8(take1(n_hl, home & ~1)[h, e]), 0)
            return pl.multiple_of(e * 2 * cs + first, 8)

        def pack(o, h, m, lo, size):
            home = me ^ m
            return jnp.concatenate([lax.dynamic_slice(o, (start_of(h, home, e) + lo, 0), (size, d)) for e in range(epd)])

        def far_rows(o, h, m, lo, size):
            return lax.ppermute(pack(o, h, m, lo, size), 'expert', perm[m])

        zero = jnp.zeros((1,), i32)
        xs = _gather(x_sib, zero, t, l_sib, c_sib)
        o_sib = _ffn(xs, w1, w3, w2, _meta(c_sib, cs // SB), epd * cs, hint)
        r_sib = lax.ppermute(o_sib, 'expert', perm[1])
        out, o_far, r_far = [o_sib], [], []
        for h in range(2):
            lst, out = lax.optimization_barrier((l_far[h], out))
            xs = _gather(x_h[h], (far >> 1)[None], 2 * half, lst, c_far[h])
            last = _ffn(xs, w1, w3, w2, _meta(c_far[h], 2 * cs // SB), epd * 2 * cs + SB, hint)
            o_far.append(last)
            out = [pack(last, h, m, 0, CAP) for m in (2, 3)]
            r_far.append([lax.ppermute(o, 'expert', perm[m]) for o, m in zip(out, (2, 3))])
        lst, out, r_far[0] = lax.optimization_barrier((l_own, out, r_far[0]))
        xs = _gather(x, zero, t, lst, c_own)
        o_own = _ffn(xs, w1, w3, w2, _meta(c_own, cs // SB), epd * cs, hint)

        k8 = jnp.arange(e_all, dtype=i32)
        slot_e = (lax.div(k8, epd) ^ me) * epd + lax.rem(k8, epd)
        by_slot = lambda a: jnp.sum(jnp.where((slot_e[:, None] == ids[None, :])[:, :, None], a[None], 0), axis=1)
        is_far = (k8 >= 2 * epd)[:, None]
        chunk_h = (ch >= hc)[None, :]
        s_n = by_slot(take1(n_h, me).T)
        base = jnp.where(is_far & chunk_h, s_n[:, :1], 0)
        held = jnp.where(is_far, jnp.where(chunk_h, s_n[:, 1:], s_n[:, :1]), s_n[:, :1] + s_n[:, 1:])
        lo = jnp.minimum((by_slot(my_off) - base) & ~15, jnp.where(is_far, CAP, cs) - CWIN)
        s_rank = by_slot(rank).reshape(e_all, nc, LANES) - base[:, :, None] - lo[:, :, None]
        s_hit = by_slot(my_hit.reshape(e_all, t)).reshape(e_all, nc, LANES) > 0
        loc = jnp.where(s_hit, s_rank, -1).reshape(e_all, t).T
        gates = jnp.sum(jnp.where(idx[:, :, None] == slot_e, g[:, :, None], 0.0), axis=1)
        arrays = (o_own, r_sib, *r_far[0], *r_far[1])

        def fast(arrays):
            return _combine(lo.T.reshape(-1), (held - lo).T.reshape(-1), loc, gates, arrays, x.dtype)

        def slow(arrays):
            buf = jnp.concatenate(arrays + (jnp.zeros((buf_rows - over_base, d), x.dtype),))

            def more(step, buf):
                for h in range(2):
                    for i, m in enumerate((2, 3)):
                        first = CAP + step * MORE
                        got = far_rows(o_far[h], h, m, first, MORE)
                        for e in range(epd):
                            row = over_base + ((2 * h + i) * epd + e) * extra + first - CAP
                            buf = lax.dynamic_update_slice(buf, got[e * MORE:(e + 1) * MORE], (row, 0))
                return buf

            buf = lax.fori_loop(0, steps, more, buf)
            op = buf.at[pos.reshape(-1)].get(mode='promise_in_bounds').reshape(k, t, d)
            return jnp.sum(g.T[:, :, None] * op.astype(jnp.float32), axis=0).astype(x.dtype)

        return lax.cond(steps > 0, slow, fast, arrays)

    tok = P(('data', 'expert'), None)
    wsp = P('expert', None, None)
    return jax.shard_map(local, mesh=mesh, in_specs=(tok, tok, P(), wsp, wsp, wsp), out_specs=tok, check_vma=False)
```

```python
import functools

import jax
import jax.numpy as jnp
from jax import lax
from jax.experimental import pallas as pl
from jax.experimental.pallas import tpu as pltpu
from jax.sharding import PartitionSpec as P

VMEM_BYTES = 67043328
LANES = 128
SB = 1024
GRAN = 128
UNIT = 512
TAILS = (128, 256, 384)
CHUNK = 256
WIN = 512
CWIN = 144
CAP = 416
MORE = 152
BN1 = 256
BN2 = 256
AHEAD = 2


def _for_rows(count, fn):
    unit = UNIT // GRAN
    whole = lax.div(count, unit)

    def body(i, c):
        fn(pl.multiple_of(i * UNIT, UNIT), UNIT)
        return c

    lax.fori_loop(0, whole, body, 0)
    rest = count - whole * unit
    for tail in TAILS:
        @pl.when(rest == tail // GRAN)
        def _():
            fn(pl.multiple_of(whole * UNIT, UNIT), tail)


def _ffn_kernel(blk, sub, ex, live, x_hbm, w1, w3, w2, o_hbm, xb, hb, wu, wd, ob, xsem, s1, s3, sd, so):
    n1, n2 = w1.shape[2] // BN1, w2.shape[2] // BN2
    count_live = live[0]

    def x_copy(s, slot):
        rows = pl.ds(pl.multiple_of(blk[s] * SB, SB), SB)
        return pltpu.make_async_copy(x_hbm.at[rows, :], xb.at[slot], xsem.at[slot])

    def up_copies(s, t, slot):
        cols = pl.ds(pl.multiple_of(t * BN1, BN1), BN1)
        return (pltpu.make_async_copy(w1.at[ex[s], :, cols], wu.at[slot, 0], s1.at[slot]),
                pltpu.make_async_copy(w3.at[ex[s], :, cols], wu.at[slot, 1], s3.at[slot]))

    def down_copy(s, t, slot):
        cols = pl.ds(pl.multiple_of(t * BN2, BN2), BN2)
        return pltpu.make_async_copy(w2.at[ex[s], :, cols], wd.at[slot], sd.at[slot])

    def out_copy(s, t, slot):
        rows = pl.ds(pl.multiple_of(blk[s] * SB, SB), SB)
        cols = pl.ds(pl.multiple_of(t * BN2, BN2), BN2)
        return pltpu.make_async_copy(ob.at[slot], o_hbm.at[rows, cols], so.at[slot])

    @pl.when(count_live > 0)
    def _():
        x_copy(0, 0).start()
        for t in range(AHEAD):
            for c in up_copies(0, t, t):
                c.start()

    def superblock(s, carry):
        count = sub[s]
        side = s & 1
        for t in range(AHEAD):
            down_copy(s, t, lax.rem(s * n2 + t, AHEAD + 1)).start()

        @pl.when(s + 1 < count_live)
        def _():
            x_copy(s + 1, 1 - side).start()
        x_copy(s, side).wait()

        def up_step(t, carry):
            step = s * n1 + t
            slot = lax.rem(step, AHEAD + 1)
            for c in up_copies(s, t, slot):
                c.wait()
            end = t >= n1 - AHEAD
            ns, nt = jnp.where(end, s + 1, s), jnp.where(end, t + AHEAD - n1, t + AHEAD)

            @pl.when(ns < count_live)
            def _():
                for c in up_copies(ns, nt, lax.rem(step + AHEAD, AHEAD + 1)):
                    c.start()
            col = pl.multiple_of(t * BN1, BN1)

            def up(r, m):
                x = xb[side, pl.ds(r, m), :]
                a = jnp.dot(x, wu[slot, 0], preferred_element_type=jnp.float32)
                b = jnp.dot(x, wu[slot, 1], preferred_element_type=jnp.float32)
                hb[pl.ds(r, m), pl.ds(col, BN1)] = (a * jax.nn.sigmoid(a) * b).astype(hb.dtype)
            _for_rows(count, up)
            return carry

        lax.fori_loop(0, n1, up_step, 0)

        def down_step(t, carry):
            slot = t & 1
            here = lax.rem(s * n2 + t, AHEAD + 1)
            down_copy(s, t, here).wait()

            @pl.when(t + AHEAD < n2)
            def _():
                down_copy(s, t + AHEAD, lax.rem(s * n2 + t + AHEAD, AHEAD + 1)).start()

            @pl.when(t >= 2)
            def _():
                out_copy(s, t - 2, slot).wait()

            def down(r, m):
                o = jnp.dot(hb[pl.ds(r, m), :], wd[here], preferred_element_type=jnp.float32)
                ob[slot, pl.ds(r, m), :] = o.astype(ob.dtype)
            _for_rows(count, down)
            out_copy(s, t, slot).start()
            return carry

        lax.fori_loop(0, n2, down_step, 0)
        out_copy(s, n2 - 2, 0).wait()
        out_copy(s, n2 - 1, 1).wait()
        return carry

    lax.fori_loop(0, count_live, superblock, 0)


def _ffn(xs, w1, w3, w2, meta, rows_out, rows_hint):
    d, f = w1.shape[1], w1.shape[2]
    smem = pl.BlockSpec(memory_space=pltpu.SMEM)
    hbm = pl.BlockSpec(memory_space=pl.ANY)
    two = pltpu.SemaphoreType.DMA((2,))
    ring = pltpu.SemaphoreType.DMA((AHEAD + 1,))
    return pl.pallas_call(
        _ffn_kernel,
        out_shape=jax.ShapeDtypeStruct((rows_out, d), xs.dtype),
        in_specs=[smem] * 4 + [hbm] * 4,
        out_specs=hbm,
        scratch_shapes=[
            pltpu.VMEM((2, SB, d), xs.dtype), pltpu.VMEM((SB, f), xs.dtype), pltpu.VMEM((AHEAD + 1, 2, d, BN1), xs.dtype),
            pltpu.VMEM((AHEAD + 1, f, BN2), xs.dtype), pltpu.VMEM((2, SB, BN2), xs.dtype), two, ring, ring, ring, two],
        compiler_params=pltpu.CompilerParams(vmem_limit_bytes=VMEM_BYTES),
        cost_estimate=pl.CostEstimate(
            flops=6 * rows_hint * d * f, bytes_accessed=12 * d * f, transcendentals=rows_hint * f),
        name="ffn",
    )(*meta, xs, w1, w3, w2)


def _pad8(n):
    return (n + 7) & ~7


def _row_list(incl, off, end, rows):
    c = incl.shape[0]
    r = lax.broadcasted_iota(jnp.int32, (rows, 1), 0)
    chunk = jnp.sum((end[None, :] <= r).astype(jnp.int32), axis=1, keepdims=True)
    hot = chunk == jnp.arange(c, dtype=jnp.int32)[None, :]
    start = jnp.sum(jnp.where(hot, off[None, :], 0), axis=1, keepdims=True)
    cum = jnp.dot(hot.astype(jnp.bfloat16), incl.astype(jnp.bfloat16), preferred_element_type=jnp.float32)
    lane = jnp.sum((cum <= (r - start).astype(jnp.float32)).astype(jnp.int32), axis=1, keepdims=True)
    return jnp.minimum(chunk * LANES + lane, c * LANES - 1)


def _blocks(counts, per, size):
    epd = counts.shape[0]
    i = jnp.arange(epd * per, dtype=jnp.int32)
    n = jnp.broadcast_to(counts[:, None], (epd, per)).reshape(-1)
    rows = jnp.clip(n - lax.rem(i, per) * size, 0, size)
    live = rows > 0
    slot = jnp.sum((live[None, :] & (i[None, :] < i[:, None])).astype(jnp.int32), axis=1)
    live_n = jnp.sum(live.astype(jnp.int32))
    put = (slot[None, :] == jnp.minimum(i, live_n - 1)[:, None]) & live[None, :]
    pick = lambda v: jnp.sum(jnp.where(put, v[None, :], 0), axis=1).astype(jnp.int32)
    return pick(i), pick(rows), pick(lax.div(i, per)), live_n[None]


def _meta(counts, per):
    blk, rows, ex, live = _blocks(counts, per, SB)
    return blk, lax.div(rows + GRAN - 1, GRAN), ex, live


def _gather_kernel(src, blk, first, last, live, list_ref, x_ref, o_ref, acc):
    i = pl.program_id(0)

    @pl.when(i < live[0])
    def _():
        lst = list_ref[...]
        acc[...] = jnp.zeros_like(acc)

        def window(w, c):
            lo = pl.multiple_of(w * WIN, WIN)
            lane = lax.broadcasted_iota(jnp.int32, (CHUNK, WIN), 1) + lo
            hot = jnp.where(lst == lane, 1.0, 0.0).astype(x_ref.dtype)
            acc[...] += jnp.dot(hot, x_ref[pl.ds(lo, WIN), :], preferred_element_type=jnp.float32)
            return c

        lax.fori_loop(lax.div(first[i], WIN), lax.div(last[i], WIN) + 1, window, 0)
        o_ref[...] = acc[...].astype(o_ref.dtype)


def _gather(x, src, tokens, lists, counts):
    rows, d = lists.shape[0], x.shape[1]
    per = rows // CHUNK // counts.shape[0]
    blk, cnt, _, live = _blocks(counts, per, CHUNK)
    table = lists.reshape(rows // CHUNK, CHUNK)
    at = blk[:, None] == jnp.arange(rows // CHUNK, dtype=jnp.int32)[None, :]
    lo = jnp.sum(jnp.where(at, table[:, 0][None, :], 0), axis=1)
    lane = jnp.arange(CHUNK, dtype=jnp.int32)[None, :]
    full = jnp.clip(jnp.broadcast_to(counts[:, None], (counts.shape[0], per)).reshape(-1)
                    - lax.rem(jnp.arange(rows // CHUNK, dtype=jnp.int32), per) * CHUNK, 0, CHUNK)
    top = jnp.max(jnp.where(lane < full[:, None], table, 0), axis=1)
    hi = jnp.sum(jnp.where(at, top[None, :], 0), axis=1)
    return pl.pallas_call(
        _gather_kernel,
        out_shape=jax.ShapeDtypeStruct((rows, d), x.dtype),
        grid_spec=pltpu.PrefetchScalarGridSpec(
            num_scalar_prefetch=5,
            grid=(rows // CHUNK,),
            in_specs=[pl.BlockSpec((CHUNK, 1), lambda i, src, blk, lo, hi, live: (blk[i], 0)),
                      pl.BlockSpec((tokens, d), lambda i, src, blk, lo, hi, live: (src[0], 0))],
            out_specs=pl.BlockSpec((CHUNK, d), lambda i, src, blk, lo, hi, live: (blk[i], 0)),
            scratch_shapes=[pltpu.VMEM((CHUNK, d), jnp.float32)],
        ),
        compiler_params=pltpu.CompilerParams(vmem_limit_bytes=VMEM_BYTES, dimension_semantics=("arbitrary",)),
        cost_estimate=pl.CostEstimate(flops=6 * rows * WIN * d, bytes_accessed=4 * tokens * d, transcendentals=0),
        name="rows",
    )(src, blk, lo, hi, live, lists, x)


def _combine_kernel(lo, cnt, loc_ref, g_ref, own, sib, f00, f01, f10, f11, y_ref, win, sem):
    b, nb = pl.program_id(0), pl.num_programs(0)
    slots = loc_ref.shape[1]
    epd = slots // 4
    d = y_ref.shape[1]

    def copy(ref, stride, b, k, side):
        row = pl.multiple_of((k % epd) * stride + lo[b * slots + k], 16)
        return pltpu.make_async_copy(ref.at[pl.ds(row, CWIN), :], win.at[side, k], sem.at[side, k])

    def start(b, side):
        stride = own.shape[0] // epd
        for k in range(2 * epd):
            copy(own if k < epd else sib, stride, b, k, side).start()
        for h, pair in enumerate(((f00, f01), (f10, f11))):
            @pl.when((b >= nb // 2) == (h == 1))
            def _():
                for k in range(2 * epd, slots):
                    copy(pair[k // epd - 2], CAP, b, k, side).start()

    side = b & 1

    @pl.when(b == 0)
    def _():
        start(0, 0)

    @pl.when(b + 1 < nb)
    def _():
        start(b + 1, 1 - side)

    for k in range(slots):
        copy(own if k < 2 * epd else f00, 0, b, k, side).wait()

    row = lax.broadcasted_iota(jnp.int32, (LANES, CWIN), 1)
    hots = [jnp.where(loc_ref[:, k:k + 1] == row, 1.0, 0.0).astype(y_ref.dtype) for k in range(slots)]
    step = 512

    def columns(c, carry):
        cols = pl.ds(pl.multiple_of(c * step, step), step)
        y = jnp.zeros((LANES, step), jnp.float32)
        r = lax.broadcasted_iota(jnp.int32, (CWIN, step), 0)
        for k in range(slots):
            w = win[side, k, :, cols].astype(jnp.float32)
            w = jnp.where(r < cnt[b * slots + k], w, 0.0).astype(win.dtype)
            y += g_ref[:, k:k + 1] * jnp.dot(hots[k], w, preferred_element_type=jnp.float32)
        y_ref[:, cols] = y.astype(y_ref.dtype)
        return carry

    lax.fori_loop(0, d // step, columns, 0)


def _combine(lo, cnt, loc, gates, arrays, dtype):
    t, slots = loc.shape
    d = arrays[0].shape[1]
    hbm = pl.BlockSpec(memory_space=pl.ANY)
    return pl.pallas_call(
        _combine_kernel,
        out_shape=jax.ShapeDtypeStruct((t, d), dtype),
        grid_spec=pltpu.PrefetchScalarGridSpec(
            num_scalar_prefetch=2,
            grid=(t // LANES,),
            in_specs=[pl.BlockSpec((LANES, slots), lambda b, lo, cnt: (b, 0))] * 2 + [hbm] * 6,
            out_specs=pl.BlockSpec((LANES, d), lambda b, lo, cnt: (b, 0)),
            scratch_shapes=[pltpu.VMEM((2, slots, CWIN, d), dtype), pltpu.SemaphoreType.DMA((2, slots))],
        ),
        compiler_params=pltpu.CompilerParams(vmem_limit_bytes=VMEM_BYTES, dimension_semantics=("arbitrary",)),
        name="combine",
    )(lo, cnt, loc, gates, *arrays)


def solution(mesh):
    n = mesh.shape['expert']

    def local(x, idx, wr, w1, w3, w2):
        t, d = x.shape
        k = idx.shape[1]
        e_all = wr.shape[1]
        epd = w1.shape[0]
        cs = 2 * k * t // e_all
        half = t // 2
        nc = t // LANES
        hc = nc // 2
        me = lax.axis_index('expert')
        sib = me ^ 1
        far = (me ^ 2) & ~1
        i32 = jnp.int32

        idx_t = idx.T
        idx_g = lax.all_gather(idx_t, ('data', 'expert'))
        xg, idx_g = lax.optimization_barrier((x, idx_g))
        idx_all = lax.dynamic_slice_in_dim(idx_g, lax.axis_index('data') * n, n, axis=0)
        x_h = [lax.all_gather(xg[h * half:(h + 1) * half], 'expert', tiled=True) for h in range(2)]
        x_sib = lax.ppermute(x, 'expert', [(i, i + 1 - 2 * (i % 2)) for i in range(n)])

        ids = jnp.arange(e_all, dtype=i32)
        hit = jnp.any(idx_all[:, None, :, :] == ids[None, :, None, None], axis=2)
        hit = hit.reshape(n, e_all, nc, LANES)
        lane = jnp.arange(LANES, dtype=i32)
        tri = (lane[:, None] <= lane[None, :]).astype(jnp.bfloat16)
        incl = jnp.dot(hit.astype(jnp.bfloat16), tri, preferred_element_type=jnp.float32).astype(i32)
        tot = incl[..., LANES - 1]
        ch = jnp.arange(nc, dtype=i32)
        off = jnp.sum(jnp.where(ch[None, :] < ch[:, None], tot[:, :, None, :], 0), axis=3)
        n_h = jnp.stack([jnp.sum(tot[..., :hc], axis=-1), jnp.sum(tot[..., hc:], axis=-1)], axis=1)

        dev = jnp.arange(n, dtype=i32)
        e_dev = lax.div(ids, epd)
        own = e_dev == me
        far_e = (e_dev >> 1) != (me >> 1)
        extra = cs - CAP
        far_base = 2 * epd * cs
        over_base = far_base + 2 * 2 * epd * CAP
        buf_rows = -(-(over_base + 2 * 2 * epd * extra) // SB) * SB

        take1 = lambda a, i: lax.dynamic_index_in_dim(a, i, 0, keepdims=False)
        mine = lambda a: lax.dynamic_slice_in_dim(a, me * epd, epd, axis=1)

        my_off, my_incl = take1(off, me), take1(incl, me)
        my_hit = take1(hit, me).astype(i32)
        rank = (my_incl - my_hit + my_off[:, :, None]).reshape(e_all, t)
        incl_l, off_l, tot_l = mine(incl), mine(off), mine(tot)
        n_hl = lax.dynamic_slice_in_dim(n_h, me * epd, epd, axis=2)

        def one_source(s):
            a, o, tt = take1(incl_l, s), take1(off_l, s), take1(tot_l, s)
            return jnp.concatenate([_row_list(a[e], o[e], o[e] + tt[e], cs) for e in range(epd)]), take1(n_hl, s).sum(axis=0)

        def far_half(h):
            sl = slice(h * hc, (h + 1) * hc)
            pick = lambda a: jnp.moveaxis(lax.dynamic_slice_in_dim(a, far, 2, axis=0)[:, :, sl], 0, 1)
            a, tt = pick(incl_l), pick(tot_l)
            cnt = lax.dynamic_slice_in_dim(n_hl, far, 2, axis=0)[:, h]
            o = pick(off_l) - (lax.dynamic_slice_in_dim(n_hl, far, 2, axis=0)[:, 0].T[:, :, None] if h else 0)
            p0 = _pad8(cnt[0])
            o = o + jnp.stack([jnp.zeros_like(p0), p0], axis=1)[:, :, None]
            o = o.reshape(epd, nc)
            end = jnp.concatenate([o[:, 1:], (p0 + cnt[1])[:, None]], axis=1)
            a = a.reshape(epd, nc, LANES)
            lst = jnp.concatenate([_row_list(a[e], o[e], end[e], 2 * cs) for e in range(epd)])
            return lst, p0 + cnt[1]

        l_own, c_own = one_source(me)
        l_sib, c_sib = one_source(sib)
        l_far, c_far = zip(far_half(0), far_half(1))

        logits = jnp.dot(x, wr, preferred_element_type=jnp.float32)
        g = jax.nn.softmax(jnp.sum(jnp.where(idx[:, :, None] == ids, logits[:, None, :], 0.0), axis=2), axis=-1)

        hint = t * k * n // e_all * epd // 4
        perm = {m: [(i, i ^ m) for i in range(n)] for m in (1, 2, 3)}

        hit_g = jnp.any(idx_g[:, None, :, :] == ids[:, None, None], axis=2)
        most = jnp.max(jnp.sum(hit_g.reshape(-1, 2, half).astype(i32), axis=2))
        steps = jnp.maximum(lax.div(most - CAP + MORE - 1, MORE), 0)

        def start_of(h, home, e):
            first = jnp.where((home & 1) == 1, _pad8(take1(n_hl, home & ~1)[h, e]), 0)
            return pl.multiple_of(e * 2 * cs + first, 8)

        def pack(o, h, m, lo, size):
            home = me ^ m
            return jnp.concatenate([lax.dynamic_slice(o, (start_of(h, home, e) + lo, 0), (size, d)) for e in range(epd)])

        def far_rows(o, h, m, lo, size):
            return lax.ppermute(pack(o, h, m, lo, size), 'expert', perm[m])

        zero = jnp.zeros((1,), i32)
        xs = _gather(x_sib, zero, t, l_sib, c_sib)
        o_sib = _ffn(xs, w1, w3, w2, _meta(c_sib, cs // SB), epd * cs, hint)
        out, o_far, r_far = [o_sib], [], []
        for h in range(2):
            lst, out = lax.optimization_barrier((l_far[h], out))
            xs = _gather(x_h[h], (far >> 1)[None], 2 * half, lst, c_far[h])
            last = _ffn(xs, w1, w3, w2, _meta(c_far[h], 2 * cs // SB), epd * 2 * cs + SB, hint)
            o_far.append(last)
            out = [pack(last, h, m, 0, CAP) for m in (2, 3)]
            r_far.append([lax.ppermute(o, 'expert', perm[m]) for o, m in zip(out, (2, 3))])
        lst, out, r_far[0], o_home = lax.optimization_barrier((l_own, out, r_far[0], o_sib))
        r_sib = lax.ppermute(o_home, 'expert', perm[1])
        xs = _gather(x, zero, t, lst, c_own)
        o_own = _ffn(xs, w1, w3, w2, _meta(c_own, cs // SB), epd * cs, hint)

        k8 = jnp.arange(e_all, dtype=i32)
        slot_e = (lax.div(k8, epd) ^ me) * epd + lax.rem(k8, epd)
        by_slot = lambda a: jnp.sum(jnp.where((slot_e[:, None] == ids[None, :])[:, :, None], a[None], 0), axis=1)
        is_far = (k8 >= 2 * epd)[:, None]
        chunk_h = (ch >= hc)[None, :]
        s_n = by_slot(take1(n_h, me).T)
        base = jnp.where(is_far & chunk_h, s_n[:, :1], 0)
        held = jnp.where(is_far, jnp.where(chunk_h, s_n[:, 1:], s_n[:, :1]), s_n[:, :1] + s_n[:, 1:])
        lo = jnp.minimum((by_slot(my_off) - base) & ~15, jnp.where(is_far, CAP, cs) - CWIN)
        s_rank = by_slot(rank).reshape(e_all, nc, LANES) - base[:, :, None] - lo[:, :, None]
        s_hit = by_slot(my_hit.reshape(e_all, t)).reshape(e_all, nc, LANES) > 0
        loc = jnp.where(s_hit, s_rank, -1).reshape(e_all, t).T
        gates = jnp.sum(jnp.where(idx[:, :, None] == slot_e, g[:, :, None], 0.0), axis=1)
        arrays = (o_own, r_sib, *r_far[0], *r_far[1])

        def fast(arrays):
            return _combine(lo.T.reshape(-1), (held - lo).T.reshape(-1), loc, gates, arrays, x.dtype)

        def slow(arrays):
            my_n0 = take1(n_h, me)[0]
            second = (jnp.arange(t, dtype=i32) >= half)[None, :]
            cross = ((e_dev ^ me) & 1) == 1
            slot = cross.astype(i32) * epd + lax.rem(ids, epd)
            far_rank = rank - jnp.where(second, my_n0[:, None], 0)
            far_slot = second.astype(i32) * 2 * epd + slot[:, None]
            far_place = jnp.where(far_rank < CAP, far_base + far_slot * CAP + far_rank,
                                  over_base + far_slot * extra + far_rank - CAP)
            near_place = jnp.where(own, lax.rem(ids, epd), epd + lax.rem(ids, epd))[:, None] * cs + rank
            place = jnp.where(far_e[:, None], far_place, near_place)
            pos = jnp.sum(jnp.where(idx_t[:, None, :] == ids[None, :, None], place[None], 0), axis=1)
            buf = jnp.concatenate(arrays + (jnp.zeros((buf_rows - over_base, d), x.dtype),))

            def more(step, buf):
                for h in range(2):
                    for i, m in enumerate((2, 3)):
                        first = CAP + step * MORE
                        got = far_rows(o_far[h], h, m, first, MORE)
                        for e in range(epd):
                            row = over_base + ((2 * h + i) * epd + e) * extra + first - CAP
                            buf = lax.dynamic_update_slice(buf, got[e * MORE:(e + 1) * MORE], (row, 0))
                return buf

            buf = lax.fori_loop(0, steps, more, buf)
            op = buf.at[pos.reshape(-1)].get(mode='promise_in_bounds').reshape(k, t, d)
            return jnp.sum(g.T[:, :, None] * op.astype(jnp.float32), axis=0).astype(x.dtype)

        return lax.cond(steps > 0, slow, fast, arrays)

    tok = P(('data', 'expert'), None)
    wsp = P('expert', None, None)
    return jax.shard_map(local, mesh=mesh, in_specs=(tok, tok, P(), wsp, wsp, wsp), out_specs=tok, check_vma=False)
```
